32 devices in a mesh: blk: 2 (over core), dp: 16 (over z, y, x).
Axes of the slice: x: 2, y: 2, z: 4, core: 2. Of those that a mesh axis runs over, the one named last changes fastest.
Arguments:
- queries: bfloat16 [4096, 256], P(('blk', 'dp')), may hold values from -1 to 1, as said below
- items: bfloat16 [4096, 256], P(('blk', 'dp')), may hold values from -1 to 1, as said below
Outputs:
- loss: float32 [], replicated
- question_slope: float32 [4096, 256], P(('blk', 'dp'))
- candidate_slope: float32 [4096, 256], P(('blk', 'dp'))
The draws below stay inside these ranges and needn't reach their ends.
Inputs may be any that keep to these rules, and one draw needn't show every extreme that they name: queries: entries lie between -1 and 1 and no row is zero; each query is close to its own item and to one item of the batch chosen by a random permutation (which may be its own). items: entries lie between -1 and 1 and no row is zero.
All inputs are finite; a program needn't handle non-finite values.
Results may differ from the reference program's by a relative error of at most 0.008.
Values may be sent and summed in bfloat16 or wider, within the bound.
A program may use at most 64 MiB of HBM per device.

```python
import jax
import jax.numpy as jnp
from jax import lax

ROWS = 128
D = 256
BATCH = 4096


def pair_draw(key):
    items_raw = jax.random.truncated_normal(jax.random.fold_in(key, 11), -4.0, 4.0, (BATCH, D), jnp.float32) * 0.0625
    partner = jax.random.permutation(jax.random.fold_in(key, 12), BATCH)
    noise_part = jax.random.truncated_normal(jax.random.fold_in(key, 13), -4.0, 4.0, (BATCH, D), jnp.float32) * 0.0625
    mixture = 0.6 * items_raw + 0.6 * items_raw[partner] + 0.7 * noise_part
    return (mixture, items_raw)


def draw_queries(key, part):
    return pair_draw(key)[0].astype(jnp.bfloat16)


def draw_items(key, part):
    return pair_draw(key)[1].astype(jnp.bfloat16)


def setup_inputs(seed: int = 0) -> dict:
    seeds = jax.random.split(jax.random.key(seed), 3)
    queries = draw_queries(jax.random.fold_in(seeds[2], 71), 0)
    items = draw_items(jax.random.fold_in(seeds[2], 71), 0)
    return dict(queries=queries, items=items)


softmax_sharpness = 0.05
tiny_square = 1e-12

def unit_rows(matrix):
    widened = matrix.astype(jnp.float32)
    length = jnp.sqrt(lax.optimization_barrier(jnp.sum(widened * widened, axis=1, keepdims=True)) + tiny_square)
    return (widened / length, length)

def round_wide(values):
    return lax.optimization_barrier(values.astype(jnp.bfloat16)).astype(jnp.float32)

def direction_slope(grad, unit, length):
    along = lax.optimization_barrier(jnp.sum(unit * grad, axis=1, keepdims=True))
    return (grad - unit * along) / length

def reference(queries, items):
    question_direction, question_magnitude = unit_rows(queries)
    candidate_direction, candidate_magnitude = unit_rows(items)
    question_gathered_all = round_wide(question_direction)
    candidate_gathered_all = round_wide(candidate_direction)
    matching_score = lax.optimization_barrier(jnp.sum(question_gathered_all * candidate_gathered_all, axis=1)) / softmax_sharpness
    q_blocks = question_gathered_all.reshape(BATCH // ROWS, ROWS, D)

    def per_block(candidate_count_overall, question_portion):
        similarity_scores = jnp.dot(question_portion, candidate_gathered_all.T, precision=lax.Precision.HIGHEST) / softmax_sharpness
        new_peak = lax.optimization_barrier(jnp.max(similarity_scores, axis=1))
        log_norm = new_peak + jnp.log(lax.optimization_barrier(jnp.sum(jnp.exp(similarity_scores - new_peak[:, None]), axis=1)))
        weights = round_wide(jnp.exp(similarity_scores - log_norm[:, None]))
        question_count_overall = jnp.dot(weights, candidate_gathered_all, precision=lax.Precision.HIGHEST)
        candidate_count_overall = candidate_count_overall + jnp.dot(weights.T, question_portion, precision=lax.Precision.HIGHEST)
        return (candidate_count_overall, (log_norm, question_count_overall))
    candidate_count_overall, (log_norm, question_count_overall) = lax.scan(per_block, jnp.zeros((BATCH, D), jnp.float32), q_blocks)
    log_norm = log_norm.reshape(BATCH)
    question_count_overall = question_count_overall.reshape(BATCH, D)
    loss = jnp.mean(log_norm - matching_score)
    question_slope = direction_slope((question_count_overall - candidate_gathered_all) / softmax_sharpness, question_direction, question_magnitude)
    candidate_slope = direction_slope((candidate_count_overall - question_gathered_all) / softmax_sharpness, candidate_direction, candidate_magnitude)
    return (loss, question_slope, candidate_slope)
```

```python
import functools
import math

import jax
import jax.numpy as jnp
from jax import lax
from jax.experimental import pallas as pl
from jax.experimental.pallas import tpu as pltpu
from jax.sharding import PartitionSpec as P

MESH = pl.DeviceIdType.MESH

softmax_sharpness = 0.05
tiny_square = 1e-12
exponent_scale = math.log2(math.e) / softmax_sharpness


def unit_rows(matrix):
    widened = matrix.astype(jnp.float32)
    length = jnp.sqrt(jnp.sum(widened * widened, axis=1, keepdims=True) + tiny_square)
    return (widened / length, length)


def direction_slope(grad, unit, length):
    along = jnp.sum(unit * grad, axis=1, keepdims=True)
    return (grad - unit * along) / length


def folded(vector, lanes):
    pieces = [vector[:, i : i + lanes] for i in range(0, vector.shape[1], lanes)]
    return functools.reduce(jnp.add, pieces)


def kernel(
    inner,
    outer,
    cores,
    batch,
    q_hbm,
    v_hbm,
    loss_ref,
    q_out,
    v_out,
    q_raw,
    v_raw,
    q_all,
    v_all,
    weights,
    sums_all,
    totals,
    losses,
    q_part,
    v_part,
    q_in,
    v_in,
    in_sem,
    qs_send,
    qs_recv,
    vs_send,
    vs_recv,
    sum_send,
    sum_recv,
    loss_send,
    loss_recv,
    qr_send,
    qr_recv,
    vr_send,
    vr_recv,
):
    core = lax.axis_index("blk")
    spot = lax.axis_index("dp")
    across = lax.rem(spot, inner)
    along = spot // inner
    members = cores * inner
    me = core * inner + across
    rows = q_hbm.shape[0]
    f32, bf16 = jnp.float32, jnp.bfloat16

    def plane_peer(k):
        other = lax.rem(me + k, members)
        return other, (other // inner, along * inner + lax.rem(other, inner))

    def line_peer(k):
        other = lax.rem(along + k, outer)
        return other, (core, other * inner + across)

    q_load = pltpu.make_async_copy(q_hbm, q_raw, in_sem.at[0])
    v_load = pltpu.make_async_copy(v_hbm, v_raw, in_sem.at[1])
    q_load.start()
    v_load.start()
    barrier = pltpu.get_barrier_semaphore()
    for k in range(1, members):
        pl.semaphore_signal(barrier, inc=1, device_id=plane_peer(k)[1], device_id_type=MESH)
    for k in range(1, outer):
        pl.semaphore_signal(barrier, inc=1, device_id=line_peer(k)[1], device_id_type=MESH)
    v_load.wait()
    v_unit, v_len = unit_rows(v_raw[...])
    v_hat = v_unit.astype(bf16)
    v_all[along] = v_hat
    q_load.wait()
    q_unit, q_len = unit_rows(q_raw[...])
    q_hat = q_unit.astype(bf16)
    q_all[me] = q_hat
    positive = jnp.sum(q_hat.astype(f32) * v_hat.astype(f32), axis=0, keepdims=True)
    pl.semaphore_wait(barrier, members + outer - 2)

    pending = []

    def send(src, dst, send_sem, recv_sem, device):
        copy = pltpu.make_async_remote_copy(
            src_ref=src,
            dst_ref=dst,
            send_sem=send_sem,
            recv_sem=recv_sem,
            device_id=device,
            device_id_type=MESH,
        )
        copy.start()
        pending.append(copy)
        return copy

    v_moves = {}
    for k in range(outer - 1, 0, -1):
        v_moves[k] = send(
            v_all.at[along], v_all.at[along], vs_send.at[k], vs_recv.at[k], line_peer(k)[1]
        )
    q_moves = {}
    for k in range(1, members):
        q_moves[k] = send(q_all.at[me], q_all.at[me], qs_send.at[k], qs_recv.at[k], plane_peer(k)[1])

    sums_all[me] = jnp.zeros(sums_all.shape[1:], f32)
    sums_all[me, pl.ds(members, 1), :] = folded(positive, sums_all.shape[2])
    for k in range(1, outer):
        v_moves[k].wait_recv()
    v_group = v_all[...].reshape(outer * rows, v_all.shape[2])

    q_own = None
    for k in range(members):
        block = lax.rem(me + members - k, members)
        if k:
            q_moves[k].wait_recv()
        scores = lax.dot_general(
            v_group, q_all[block], (((1,), (1,)), ((), ())), preferred_element_type=f32
        )
        raised = jnp.exp2(scores * exponent_scale)
        weights[block] = raised
        sums_all[me, pl.ds(block, 1), :] = jnp.sum(raised, axis=0, keepdims=True)
    for k in range(1, members):
        send(sums_all.at[me], sums_all.at[me], sum_send.at[k], sum_recv.at[k], plane_peer(k)[1])

    q_sends = {}
    for k in list(range(1, members)) + [0]:
        block, device = plane_peer(k)
        share = lax.dot_general(
            weights[block].astype(bf16), v_group, (((0,), (0,)), ((), ())), preferred_element_type=f32
        )
        if k:
            q_part[k] = share.astype(bf16)
            q_sends[k] = send(q_part.at[k], q_in.at[k], qr_send.at[k], qr_recv.at[k], device)
        else:
            q_own = share

    for copy in pending[outer - 1 + members - 1 : outer - 1 + 2 * (members - 1)]:
        copy.wait_recv()
    message = functools.reduce(jnp.add, [sums_all[i] for i in range(members)])
    total = message[:members]
    inverse = 1.0 / total
    totals[...] = inverse
    log_norm = jnp.log(total)
    gathered_loss = jnp.sum(log_norm, axis=0, keepdims=True) - message[members : members + 1] / (
        softmax_sharpness
    )
    losses[along] = jnp.broadcast_to(gathered_loss, losses.shape[1:])

    probs = [(weights[b] * inverse[b : b + 1]).astype(bf16) for b in range(members)]
    for b in range(members):
        weights_bf = probs[b]
        q_block = q_all[b]
        part = jnp.dot(weights_bf, q_block, preferred_element_type=f32)
        if b == 0:
            v_part[...] = part
        else:
            v_part[...] += part
    v_sends = {}
    v_own = None
    v_stage = v_in.at[0]
    for k in range(outer - 1, -1, -1):
        block, device = line_peer(k)
        share = v_part[pl.ds(pl.multiple_of(block * rows, rows), rows), :]
        if k:
            v_in[outer + k] = share.astype(bf16)
            v_sends[k] = send(v_in.at[outer + k], v_in.at[k], vr_send.at[k], vr_recv.at[k], device)
        else:
            v_own = share
    loss_sends = {}
    for k in range(1, outer):
        loss_sends[k] = send(
            losses.at[along], losses.at[along], loss_send.at[k], loss_recv.at[k], line_peer(k)[1]
        )

    for k in range(1, members):
        q_sends[k].wait_recv()
        q_own = q_own + q_in[k].astype(f32)
    own_inverse = jnp.transpose(jnp.broadcast_to(totals[pl.ds(me, 1), :], (rows, rows)))[:, :1]
    q_pull = (q_own * own_inverse - v_hat.astype(f32)) / softmax_sharpness
    q_out[...] = direction_slope(q_pull, q_unit, q_len)

    for k in range(1, outer):
        loss_sends[k].wait_recv()
    loss_row = functools.reduce(jnp.add, [losses[i] for i in range(outer)])
    loss_ref[...] = jnp.broadcast_to(
        jnp.sum(loss_row[:1], axis=1, keepdims=True) / batch, loss_ref.shape
    )
    for k in range(1, outer):
        v_sends[k].wait_recv()
        v_own = v_own + v_in[k].astype(f32)
    v_pull = (v_own - q_hat.astype(f32)) / softmax_sharpness
    v_out[...] = direction_slope(v_pull, v_unit, v_len)
    for copy in pending:
        copy.wait_send()


def near_square(count):
    return max(d for d in range(1, math.isqrt(count) + 1) if count % d == 0)


def solution(mesh):
    cores, spots = mesh.shape["blk"], mesh.shape["dp"]
    outer = near_square(spots)
    inner = spots // outer
    members = cores * inner

    def per_device(queries, items):
        rows, width = queries.shape
        f32, bf16 = jnp.float32, jnp.bfloat16
        lanes = rows
        note = members + 8
        dma = pltpu.SemaphoreType.DMA
        vmem = pl.BlockSpec(memory_space=pltpu.VMEM)
        anywhere = pl.BlockSpec(memory_space=pl.ANY)
        loss, q_slope, v_slope = pl.pallas_call(
            functools.partial(kernel, inner, outer, cores, rows * cores * spots),
            out_shape=(
                jax.ShapeDtypeStruct((8, 128), f32),
                jax.ShapeDtypeStruct((rows, width), f32),
                jax.ShapeDtypeStruct((rows, width), f32),
            ),
            in_specs=[anywhere, anywhere],
            out_specs=(vmem, vmem, vmem),
            scratch_shapes=[
                pltpu.VMEM((rows, width), bf16),
                pltpu.VMEM((rows, width), bf16),
                pltpu.VMEM((members, rows, width), bf16),
                pltpu.VMEM((outer, rows, width), bf16),
                pltpu.VMEM((members, outer * rows, rows), f32),
                pltpu.VMEM((members, note, lanes), f32),
                pltpu.VMEM((members, lanes), f32),
                pltpu.VMEM((outer, 8, lanes), f32),
                pltpu.VMEM((members, rows, width), bf16),
                pltpu.VMEM((outer * rows, width), f32),
                pltpu.VMEM((members, rows, width), bf16),
                pltpu.VMEM((2 * outer, rows, width), bf16),
                dma((2,)),
                dma((members,)),
                dma((members,)),
                dma((outer,)),
                dma((outer,)),
                dma((members,)),
                dma((members,)),
                dma((outer,)),
                dma((outer,)),
                dma((members,)),
                dma((members,)),
                dma((outer,)),
                dma((outer,)),
            ],
            compiler_params=pltpu.CompilerParams(
                collective_id=0, has_side_effects=True, vmem_limit_bytes=60 * 1024 * 1024
            ),
        )(queries, items)
        return loss[0, 0], q_slope, v_slope

    placed = (P(("blk", "dp"), None), P(("blk", "dp"), None))
    return jax.shard_map(
        per_device,
        mesh=mesh,
        in_specs=placed,
        out_specs=(P(), P(("blk", "dp"), None), P(("blk", "dp"), None)),
        check_vma=False,
    )
```

```python
import functools
import math

import jax
import jax.numpy as jnp
from jax import lax
from jax.experimental import pallas as pl
from jax.experimental.pallas import tpu as pltpu
from jax.sharding import PartitionSpec as P

MESH = pl.DeviceIdType.MESH

softmax_sharpness = 0.05
tiny_square = 1e-12
exponent_scale = math.log2(math.e) / softmax_sharpness


def unit_rows(matrix):
    widened = matrix.astype(jnp.float32)
    length = jnp.sqrt(jnp.sum(widened * widened, axis=1, keepdims=True) + tiny_square)
    return (widened / length, length)


def direction_slope(grad, unit, length):
    along = jnp.sum(unit * grad, axis=1, keepdims=True)
    return (grad - unit * along) / length


def folded(vector, lanes):
    pieces = [vector[:, i : i + lanes] for i in range(0, vector.shape[1], lanes)]
    return functools.reduce(jnp.add, pieces)


def partner(spot, step, count):
    if count & (count - 1):
        return lax.rem(spot + step, count)
    other = spot
    bit = 1
    while bit < count:
        if step & bit:
            other = other + bit * (1 - 2 * lax.rem(spot // bit, 2))
        bit *= 2
    return other


def source(spot, step, count):
    if count & (count - 1):
        return lax.rem(spot + count - step, count)
    return partner(spot, step, count)


def kernel(
    inner,
    outer,
    cores,
    q_hbm,
    v_hbm,
    loss_ref,
    q_out,
    v_out,
    q_raw,
    v_raw,
    q_all,
    v_all,
    weights,
    q_sum,
    sums_all,
    totals,
    losses,
    q_part,
    v_part,
    q_in,
    v_in,
    in_sem,
    qs_send,
    qs_recv,
    qf_send,
    qf_recv,
    vs_send,
    vs_recv,
    sum_send,
    sum_recv,
    loss_send,
    loss_recv,
    qr_send,
    qr_recv,
    vr_send,
    vr_recv,
):
    core = lax.axis_index("blk")
    spot = lax.axis_index("dp")
    across = lax.rem(spot, inner)
    along = spot // inner
    members = cores * inner
    me = core * inner + across
    rows = q_hbm.shape[0]
    width = q_hbm.shape[1]
    batch = rows * members * outer
    f32, bf16 = jnp.float32, jnp.bfloat16
    plane_steps = [(c, s) for s in range(inner) for c in range(cores) if c or s]
    line_steps = list(range(outer - 1, 0, -1))

    def plane_peer(step):
        c, s = step
        there_core, there = partner(core, c, cores), partner(across, s, inner)
        return there_core * inner + there, (there_core, along * inner + there)

    def plane_source(step):
        c, s = step
        return source(core, c, cores) * inner + source(across, s, inner)

    def line_peer(s):
        there = partner(along, s, outer)
        return there, (core, there * inner + across)

    def plane_key(step):
        return step[1] * cores + step[0]

    q_load = pltpu.make_async_copy(q_hbm, q_raw, in_sem.at[0])
    v_load = pltpu.make_async_copy(v_hbm, v_raw, in_sem.at[1])
    v_load.start()
    q_load.start()
    barrier = pltpu.get_barrier_semaphore()
    for s in line_steps:
        pl.semaphore_signal(barrier, inc=1, device_id=line_peer(s)[1], device_id_type=MESH)
    for step in plane_steps:
        pl.semaphore_signal(barrier, inc=1, device_id=plane_peer(step)[1], device_id_type=MESH)
    v_load.wait()
    v_unit, v_len = unit_rows(v_raw[...])
    v_hat = v_unit.astype(bf16)
    v_all[along] = v_hat
    q_load.wait()
    q_unit, q_len = unit_rows(q_raw[...])
    q_hat = q_unit.astype(bf16)
    q_all[me] = q_hat
    positive = jnp.sum(q_hat.astype(f32) * v_hat.astype(f32), axis=0, keepdims=True)
    pl.semaphore_wait(barrier, members + outer - 2)

    pending = []

    def send(src, dst, send_sem, recv_sem, device):
        copy = pltpu.make_async_remote_copy(
            src_ref=src,
            dst_ref=dst,
            send_sem=send_sem,
            recv_sem=recv_sem,
            device_id=device,
            device_id_type=MESH,
        )
        copy.start()
        pending.append(copy)
        return copy

    v_moves = {}
    for s in line_steps:
        v_moves[s] = send(
            v_all.at[along], v_all.at[along], vs_send.at[s], vs_recv.at[s], line_peer(s)[1]
        )
    q_moves = {}
    for s in range(inner - 1, 0, -1):
        q_moves[s] = send(
            q_all.at[me], q_all.at[me], qs_send.at[s], qs_recv.at[s], plane_peer((0, s))[1]
        )
    forwards = []

    def pass_on(s):
        slot = plane_source((0, s))
        for c in range(1, cores):
            key = plane_key((c, s))
            there = plane_peer((c, 0))[1]
            forwards.append(
                send(q_all.at[slot], q_all.at[slot], qf_send.at[key], qf_recv.at[key], there)
            )

    pass_on(0)
    sums_all[me] = jnp.zeros(sums_all.shape[1:], f32)
    sums_all[me, pl.ds(members, 1), :] = folded(positive, sums_all.shape[2])
    for s in range(1, inner):
        q_moves[s].wait_recv()
        pass_on(s)
    for copy in forwards:
        copy.wait_recv()
    q_group = q_all[...].reshape(members * rows, width)

    summed = None
    for n, s in enumerate([0] + line_steps[::-1]):
        if s:
            v_moves[s].wait_recv()
        slot = source(along, s, outer) if s else along
        v_block = v_all[slot]
        scores = lax.dot_general(
            v_block, q_group, (((1,), (1,)), ((), ())), preferred_element_type=f32
        )
        raised = jnp.exp2(scores * exponent_scale)
        weights[slot] = raised
        below = jnp.sum(raised, axis=0, keepdims=True)
        summed = below if summed is None else summed + below
        if n == outer - 1:
            for b in range(members):
                sums_all[me, pl.ds(b, 1), :] = summed[:, b * rows : (b + 1) * rows]
            sum_moves = {}
            for step in plane_steps:
                key = plane_key(step)
                sum_moves[step] = send(
                    sums_all.at[me],
                    sums_all.at[me],
                    sum_send.at[key],
                    sum_recv.at[key],
                    plane_peer(step)[1],
                )
        share = lax.dot_general(
            raised.astype(bf16), v_block, (((0,), (0,)), ((), ())), preferred_element_type=f32
        ).reshape(members, rows, width)
        if n == 0:
            q_sum[...] = share
        elif n < outer - 1:
            q_sum[...] += share
        else:
            q_sum[...] += share

    q_moves = {}
    for step in plane_steps[::-1]:
        key = plane_key(step)
        there, device = plane_peer(step)
        q_part[key] = q_sum[there].astype(bf16)
        q_moves[step] = send(q_part.at[key], q_in.at[key], qr_send.at[key], qr_recv.at[key], device)

    for step in plane_steps:
        sum_moves[step].wait_recv()
    message = functools.reduce(jnp.add, [sums_all[i] for i in range(members)])
    total = message[:members]
    inverse = 1.0 / total
    totals[...] = inverse
    inverse_row = jnp.concatenate([inverse[b : b + 1] for b in range(members)], axis=1)
    v_moves = {}
    for s in line_steps + [0]:
        slot, device = line_peer(s)
        probs = (weights[slot] * inverse_row).astype(bf16)
        share = jnp.dot(probs, q_group, preferred_element_type=f32)
        if s:
            v_part[s] = share.astype(bf16)
            v_moves[s] = send(v_part.at[s], v_in.at[s], vr_send.at[s], vr_recv.at[s], device)
        else:
            v_own = share
    log_norm = jnp.log(total)
    gathered_loss = (
        jnp.sum(log_norm, axis=0, keepdims=True)
        - message[members : members + 1] / softmax_sharpness
    )
    losses[along] = jnp.broadcast_to(gathered_loss, losses.shape[1:])
    loss_moves = {}
    for s in line_steps:
        loss_moves[s] = send(
            losses.at[along], losses.at[along], loss_send.at[s], loss_recv.at[s], line_peer(s)[1]
        )

    q_own = q_sum[me]
    for step in plane_steps:
        q_moves[step].wait_recv()
        q_own = q_own + q_in[plane_key(step)].astype(f32)
    own_inverse = jnp.transpose(jnp.broadcast_to(totals[pl.ds(me, 1), :], (rows, rows)))[:, :1]
    q_pull = (q_own * own_inverse - v_all[along].astype(f32)) / softmax_sharpness
    q_unit, q_len = unit_rows(q_raw[...])
    q_out[...] = direction_slope(q_pull, q_unit, q_len)

    for s in line_steps[::-1]:
        v_moves[s].wait_recv()
        v_own = v_own + v_in[s].astype(f32)
    v_pull = (v_own - q_all[me].astype(f32)) / softmax_sharpness
    v_unit, v_len = unit_rows(v_raw[...])
    v_out[...] = direction_slope(v_pull, v_unit, v_len)
    for s in line_steps:
        loss_moves[s].wait_recv()
    loss_row = functools.reduce(jnp.add, [losses[i] for i in range(outer)])
    loss_ref[0, 0] = jnp.sum(loss_row[:1]) / batch
    for copy in pending:
        copy.wait_send()


def near_square(count):
    return max(d for d in range(1, math.isqrt(count) + 1) if count % d == 0)


def solution(mesh):
    cores, spots = mesh.shape["blk"], mesh.shape["dp"]
    outer = near_square(spots)
    inner = spots // outer
    members = cores * inner

    def per_device(queries, items):
        rows, width = queries.shape
        f32, bf16 = jnp.float32, jnp.bfloat16
        lanes = rows
        note = members + 8
        dma = pltpu.SemaphoreType.DMA
        vmem = pl.BlockSpec(memory_space=pltpu.VMEM)
        anywhere = pl.BlockSpec(memory_space=pl.ANY)
        loss, q_slope, v_slope = pl.pallas_call(
            functools.partial(kernel, inner, outer, cores),
            out_shape=(
                jax.ShapeDtypeStruct((1, 1), f32),
                jax.ShapeDtypeStruct((rows, width), f32),
                jax.ShapeDtypeStruct((rows, width), f32),
            ),
            in_specs=[anywhere, anywhere],
            out_specs=(pl.BlockSpec(memory_space=pltpu.SMEM), vmem, vmem),
            scratch_shapes=[
                pltpu.VMEM((rows, width), bf16),
                pltpu.VMEM((rows, width), bf16),
                pltpu.VMEM((members, rows, width), bf16),
                pltpu.VMEM((outer, rows, width), bf16),
                pltpu.VMEM((outer, rows, members * rows), f32),
                pltpu.VMEM((members, rows, width), f32),
                pltpu.VMEM((members, note, lanes), f32),
                pltpu.VMEM((members, lanes), f32),
                pltpu.VMEM((outer, 8, lanes), f32),
                pltpu.VMEM((members, rows, width), bf16),
                pltpu.VMEM((outer, rows, width), bf16),
                pltpu.VMEM((members, rows, width), bf16),
                pltpu.VMEM((outer, rows, width), bf16),
                dma((2,)),
                dma((inner,)),
                dma((inner,)),
                dma((members,)),
                dma((members,)),
                dma((outer,)),
                dma((outer,)),
                dma((members,)),
                dma((members,)),
                dma((outer,)),
                dma((outer,)),
                dma((members,)),
                dma((members,)),
                dma((outer,)),
                dma((outer,)),
            ],
            compiler_params=pltpu.CompilerParams(
                collective_id=0, has_side_effects=True, vmem_limit_bytes=60 * 1024 * 1024
            ),
        )(queries, items)
        return loss.reshape(()), q_slope, v_slope

    placed = (P(("blk", "dp"), None), P(("blk", "dp"), None))
    return jax.shard_map(
        per_device,
        mesh=mesh,
        in_specs=placed,
        out_specs=(P(), P(("blk", "dp"), None), P(("blk", "dp"), None)),
        check_vma=False,
    )
```

```python
import functools
import math

import jax
import jax.numpy as jnp
from jax import lax
from jax.experimental import pallas as pl
from jax.experimental.pallas import tpu as pltpu
from jax.sharding import PartitionSpec as P

MESH = pl.DeviceIdType.MESH

softmax_sharpness = 0.05
tiny_square = 1e-12
exponent_scale = math.log2(math.e) / softmax_sharpness


def unit_rows(matrix):
    widened = matrix.astype(jnp.float32)
    length = jnp.sqrt(jnp.sum(widened * widened, axis=1, keepdims=True) + tiny_square)
    return (widened / length, length)


def direction_slope(grad, unit, length):
    along = jnp.sum(unit * grad, axis=1, keepdims=True)
    return (grad - unit * along) / length


def folded(vector, lanes):
    pieces = [vector[:, i : i + lanes] for i in range(0, vector.shape[1], lanes)]
    return functools.reduce(jnp.add, pieces)


def partner(spot, step, count):
    if count & (count - 1):
        return lax.rem(spot + step, count)
    other = spot
    bit = 1
    while bit < count:
        if step & bit:
            other = other + bit * (1 - 2 * lax.rem(spot // bit, 2))
        bit *= 2
    return other


def source(spot, step, count):
    if count & (count - 1):
        return lax.rem(spot + count - step, count)
    return partner(spot, step, count)


def kernel(
    inner,
    outer,
    cores,
    q_hbm,
    v_hbm,
    loss_ref,
    q_out,
    v_out,
    q_raw,
    v_raw,
    q_all,
    v_all,
    weights,
    q_sum,
    sums_all,
    totals,
    losses,
    q_part,
    v_part,
    q_in,
    v_in,
    in_sem,
    qs_send,
    qs_recv,
    qf_send,
    qf_recv,
    vs_send,
    vs_recv,
    sum_send,
    sum_recv,
    loss_send,
    loss_recv,
    qr_send,
    qr_recv,
    vr_send,
    vr_recv,
):
    core = lax.axis_index("blk")
    spot = lax.axis_index("dp")
    across = lax.rem(spot, inner)
    along = spot // inner
    members = cores * inner
    me = core * inner + across
    rows = q_hbm.shape[0]
    width = q_hbm.shape[1]
    batch = rows * members * outer
    f32, bf16 = jnp.float32, jnp.bfloat16
    plane_steps = [(c, s) for s in range(inner) for c in range(cores) if c or s]
    line_steps = list(range(outer - 1, 0, -1))

    def plane_peer(step):
        c, s = step
        there_core, there = partner(core, c, cores), partner(across, s, inner)
        return there_core * inner + there, (there_core, along * inner + there)

    def plane_source(step):
        c, s = step
        return source(core, c, cores) * inner + source(across, s, inner)

    def line_peer(s):
        there = partner(along, s, outer)
        return there, (core, there * inner + across)

    def plane_key(step):
        return step[1] * cores + step[0]

    q_load = pltpu.make_async_copy(q_hbm, q_raw, in_sem.at[0])
    v_load = pltpu.make_async_copy(v_hbm, v_raw, in_sem.at[1])
    v_load.start()
    q_load.start()
    barrier = pltpu.get_barrier_semaphore()
    for s in line_steps:
        pl.semaphore_signal(barrier, inc=1, device_id=line_peer(s)[1], device_id_type=MESH)
    for step in plane_steps:
        pl.semaphore_signal(barrier, inc=1, device_id=plane_peer(step)[1], device_id_type=MESH)
    v_load.wait()
    v_unit, v_len = unit_rows(v_raw[...])
    v_hat = v_unit.astype(bf16)
    v_all[along] = v_hat
    q_load.wait()
    q_unit, q_len = unit_rows(q_raw[...])
    q_hat = q_unit.astype(bf16)
    q_all[me] = q_hat
    positive = jnp.sum(q_hat.astype(f32) * v_hat.astype(f32), axis=0, keepdims=True)
    pl.semaphore_wait(barrier, members + outer - 2)

    pending = []

    def send(src, dst, send_sem, recv_sem, device):
        copy = pltpu.make_async_remote_copy(
            src_ref=src,
            dst_ref=dst,
            send_sem=send_sem,
            recv_sem=recv_sem,
            device_id=device,
            device_id_type=MESH,
        )
        copy.start()
        pending.append(copy)
        return copy

    v_moves = {}
    for s in line_steps:
        v_moves[s] = send(
            v_all.at[along], v_all.at[along], vs_send.at[s], vs_recv.at[s], line_peer(s)[1]
        )
    q_moves = {}
    for s in range(inner - 1, 0, -1):
        q_moves[s] = send(
            q_all.at[me], q_all.at[me], qs_send.at[s], qs_recv.at[s], plane_peer((0, s))[1]
        )
    forwards = []

    def pass_on(s):
        slot = plane_source((0, s))
        for c in range(1, cores):
            key = plane_key((c, s))
            there = plane_peer((c, 0))[1]
            forwards.append(
                send(q_all.at[slot], q_all.at[slot], qf_send.at[key], qf_recv.at[key], there)
            )

    pass_on(0)
    sums_all[me] = jnp.zeros(sums_all.shape[1:], f32)
    sums_all[me, pl.ds(members, 1), :] = folded(positive, sums_all.shape[2])
    for s in range(1, inner):
        q_moves[s].wait_recv()
        pass_on(s)
    for copy in forwards:
        copy.wait_recv()
    q_group = q_all[...].reshape(members * rows, width)

    summed = None
    for n, s in enumerate([0] + line_steps[::-1]):
        if s:
            v_moves[s].wait_recv()
        slot = source(along, s, outer) if s else along
        v_block = v_all[slot]
        scores = lax.dot_general(
            v_block, q_group, (((1,), (1,)), ((), ())), preferred_element_type=f32
        )
        raised = jnp.exp2(scores * exponent_scale)
        weights[slot] = raised
        below = jnp.sum(raised, axis=0, keepdims=True)
        summed = below if summed is None else summed + below
        if n == outer - 1:
            for b in range(members):
                sums_all[me, pl.ds(b, 1), :] = summed[:, b * rows : (b + 1) * rows]
            sum_moves = {}
            for step in plane_steps:
                key = plane_key(step)
                sum_moves[step] = send(
                    sums_all.at[me],
                    sums_all.at[me],
                    sum_send.at[key],
                    sum_recv.at[key],
                    plane_peer(step)[1],
                )
        share = lax.dot_general(
            raised.astype(bf16), v_block, (((0,), (0,)), ((), ())), preferred_element_type=f32
        ).reshape(members, rows, width)
        if n == 0:
            q_sum[...] = share
        elif n < outer - 1:
            q_sum[...] += share
        else:
            q_sum[...] += share

    q_moves = {}
    for step in plane_steps[::-1]:
        key = plane_key(step)
        there, device = plane_peer(step)
        q_part[key] = q_sum[there].astype(bf16)
        q_moves[step] = send(q_part.at[key], q_in.at[key], qr_send.at[key], qr_recv.at[key], device)

    for step in plane_steps:
        sum_moves[step].wait_recv()
    message = functools.reduce(jnp.add, [sums_all[i] for i in range(members)])
    total = message[:members]
    inverse = 1.0 / total
    totals[...] = inverse
    inverse_row = jnp.concatenate([inverse[b : b + 1] for b in range(members)], axis=1)
    v_moves = {}
    for s in line_steps + [0]:
        slot, device = line_peer(s)
        probs = (weights[slot] * inverse_row).astype(bf16)
        share = jnp.dot(probs, q_group, preferred_element_type=f32)
        if s:
            v_part[s] = share.astype(bf16)
            v_moves[s] = send(v_part.at[s], v_in.at[s], vr_send.at[s], vr_recv.at[s], device)
        else:
            v_own = share
    log_norm = jnp.log(total)
    gathered_loss = (
        jnp.sum(log_norm, axis=0, keepdims=True)
        - message[members : members + 1] / softmax_sharpness
    )
    losses[along] = jnp.broadcast_to(gathered_loss, losses.shape[1:])
    loss_moves = {}
    for s in line_steps:
        loss_moves[s] = send(
            losses.at[along], losses.at[along], loss_send.at[s], loss_recv.at[s], line_peer(s)[1]
        )

    q_own = q_sum[me]
    for step in plane_steps:
        q_moves[step].wait_recv()
        q_own = q_own + q_in[plane_key(step)].astype(f32)
    own_inverse = jnp.transpose(jnp.broadcast_to(totals[pl.ds(me, 1), :], (rows, rows)))[:, :1]
    q_pull = (q_own * own_inverse - v_all[along].astype(f32))
    q_unit, q_len = unit_rows(q_raw[...])
    q_out[...] = direction_slope(q_pull, q_unit, q_len)

    for s in line_steps[::-1]:
        v_moves[s].wait_recv()
        v_own = v_own + v_in[s].astype(f32)
    v_pull = (v_own - q_all[me].astype(f32))
    v_unit, v_len = unit_rows(v_raw[...])
    v_out[...] = direction_slope(v_pull, v_unit, v_len)
    for s in line_steps:
        loss_moves[s].wait_recv()
    loss_row = functools.reduce(jnp.add, [losses[i] for i in range(outer)])
    loss_ref[0, 0] = jnp.sum(loss_row[:1]) / batch
    for copy in pending:
        copy.wait_send()


def near_square(count):
    return max(d for d in range(1, math.isqrt(count) + 1) if count % d == 0)


def solution(mesh):
    cores, spots = mesh.shape["blk"], mesh.shape["dp"]
    outer = near_square(spots)
    inner = spots // outer
    members = cores * inner

    def per_device(queries, items):
        rows, width = queries.shape
        f32, bf16 = jnp.float32, jnp.bfloat16
        lanes = rows
        note = members + 8
        dma = pltpu.SemaphoreType.DMA
        vmem = pl.BlockSpec(memory_space=pltpu.VMEM)
        anywhere = pl.BlockSpec(memory_space=pl.ANY)
        loss, q_slope, v_slope = pl.pallas_call(
            functools.partial(kernel, inner, outer, cores),
            out_shape=(
                jax.ShapeDtypeStruct((1, 1), f32),
                pltpu.VMEM((rows, width), f32),
                pltpu.VMEM((rows, width), f32),
            ),
            in_specs=[anywhere, anywhere],
            out_specs=(pl.BlockSpec(memory_space=pltpu.SMEM), vmem, vmem),
            scratch_shapes=[
                pltpu.VMEM((rows, width), bf16),
                pltpu.VMEM((rows, width), bf16),
                pltpu.VMEM((members, rows, width), bf16),
                pltpu.VMEM((outer, rows, width), bf16),
                pltpu.VMEM((outer, rows, members * rows), f32),
                pltpu.VMEM((members, rows, width), f32),
                pltpu.VMEM((members, note, lanes), f32),
                pltpu.VMEM((members, lanes), f32),
                pltpu.VMEM((outer, 8, lanes), f32),
                pltpu.VMEM((members, rows, width), bf16),
                pltpu.VMEM((outer, rows, width), bf16),
                pltpu.VMEM((members, rows, width), bf16),
                pltpu.VMEM((outer, rows, width), bf16),
                dma((2,)),
                dma((inner,)),
                dma((inner,)),
                dma((members,)),
                dma((members,)),
                dma((outer,)),
                dma((outer,)),
                dma((members,)),
                dma((members,)),
                dma((outer,)),
                dma((outer,)),
                dma((members,)),
                dma((members,)),
                dma((outer,)),
                dma((outer,)),
            ],
            compiler_params=pltpu.CompilerParams(
                collective_id=0, has_side_effects=True, vmem_limit_bytes=60 * 1024 * 1024
            ),
        )(queries, items)
        return loss.reshape(()), q_slope / softmax_sharpness, v_slope / softmax_sharpness

    placed = (P(("blk", "dp"), None), P(("blk", "dp"), None))
    return jax.shard_map(
        per_device,
        mesh=mesh,
        in_specs=placed,
        out_specs=(P(), P(("blk", "dp"), None), P(("blk", "dp"), None)),
        check_vma=False,
    )
```

```python
import functools
import math

import jax
import jax.numpy as jnp
from jax import lax
from jax.experimental import pallas as pl
from jax.experimental.pallas import tpu as pltpu
from jax.sharding import PartitionSpec as P

MESH = pl.DeviceIdType.MESH

softmax_sharpness = 0.05
tiny_square = 1e-12
exponent_scale = math.log2(math.e) / softmax_sharpness


def unit_rows(matrix):
    widened = matrix.astype(jnp.float32)
    length = jnp.sqrt(jnp.sum(widened * widened, axis=1, keepdims=True) + tiny_square)
    return (widened / length, length)


def direction_slope(grad, unit, length):
    along = jnp.sum(unit * grad, axis=1, keepdims=True)
    return (grad - unit * along) / length


def folded(vector, lanes):
    pieces = [vector[:, i : i + lanes] for i in range(0, vector.shape[1], lanes)]
    return functools.reduce(jnp.add, pieces)


def partner(spot, step, count):
    if count & (count - 1):
        return lax.rem(spot + step, count)
    other = spot
    bit = 1
    while bit < count:
        if step & bit:
            other = other + bit * (1 - 2 * lax.rem(spot // bit, 2))
        bit *= 2
    return other


def source(spot, step, count):
    if count & (count - 1):
        return lax.rem(spot + count - step, count)
    return partner(spot, step, count)


def kernel(
    inner,
    outer,
    cores,
    q_hbm,
    v_hbm,
    loss_ref,
    q_out,
    v_out,
    q_raw,
    v_raw,
    q_all,
    v_all,
    weights,
    q_sum,
    sums_all,
    totals,
    losses,
    q_part,
    v_part,
    q_in,
    v_in,
    v_sum,
    units,
    shrink,
    in_sem,
    qs_send,
    qs_recv,
    qf_send,
    qf_recv,
    vs_send,
    vs_recv,
    sum_send,
    sum_recv,
    loss_send,
    loss_recv,
    qr_send,
    qr_recv,
    vr_send,
    vr_recv,
):
    core = lax.axis_index("blk")
    spot = lax.axis_index("dp")
    across = lax.rem(spot, inner)
    along = spot // inner
    members = cores * inner
    me = core * inner + across
    rows = q_hbm.shape[0]
    width = q_hbm.shape[1]
    batch = rows * members * outer
    f32, bf16 = jnp.float32, jnp.bfloat16
    plane_steps = [(c, s) for s in range(inner) for c in range(cores) if c or s]
    line_steps = list(range(outer - 1, 0, -1))
    arrivals = [s for s in line_steps[::-1] if s != 2] + [s for s in line_steps if s == 2]

    def plane_peer(step):
        c, s = step
        there_core, there = partner(core, c, cores), partner(across, s, inner)
        return there_core * inner + there, (there_core, along * inner + there)

    def plane_source(step):
        c, s = step
        return source(core, c, cores) * inner + source(across, s, inner)

    def line_peer(s):
        there = partner(along, s, outer)
        return there, (core, there * inner + across)

    def plane_key(step):
        return step[1] * cores + step[0]

    q_load = pltpu.make_async_copy(q_hbm, q_raw, in_sem.at[0])
    v_load = pltpu.make_async_copy(v_hbm, v_raw, in_sem.at[1])
    v_load.start()
    q_load.start()
    barrier = pltpu.get_barrier_semaphore()
    for s in line_steps:
        pl.semaphore_signal(barrier, inc=1, device_id=line_peer(s)[1], device_id_type=MESH)
    for step in plane_steps:
        pl.semaphore_signal(barrier, inc=1, device_id=plane_peer(step)[1], device_id_type=MESH)
    v_load.wait()
    v_unit, v_len = unit_rows(v_raw[...])
    v_hat = v_unit.astype(bf16)
    v_all[along] = v_hat
    q_load.wait()
    q_unit, q_len = unit_rows(q_raw[...])
    q_hat = q_unit.astype(bf16)
    q_all[me] = q_hat
    positive = jnp.sum(q_hat.astype(f32) * v_hat.astype(f32), axis=0, keepdims=True)
    pl.semaphore_wait(barrier, members + outer - 2)

    pending = []

    def send(src, dst, send_sem, recv_sem, device):
        copy = pltpu.make_async_remote_copy(
            src_ref=src,
            dst_ref=dst,
            send_sem=send_sem,
            recv_sem=recv_sem,
            device_id=device,
            device_id_type=MESH,
        )
        copy.start()
        pending.append(copy)
        return copy

    v_moves = {}
    for s in line_steps:
        v_moves[s] = send(
            v_all.at[along], v_all.at[along], vs_send.at[s], vs_recv.at[s], line_peer(s)[1]
        )
    q_moves = {}
    for s in range(inner - 1, 0, -1):
        q_moves[s] = send(
            q_all.at[me], q_all.at[me], qs_send.at[s], qs_recv.at[s], plane_peer((0, s))[1]
        )
    forwards = []

    def pass_on(s):
        slot = plane_source((0, s))
        for c in range(1, cores):
            key = plane_key((c, s))
            there = plane_peer((c, 0))[1]
            forwards.append(
                send(q_all.at[slot], q_all.at[slot], qf_send.at[key], qf_recv.at[key], there)
            )

    pass_on(0)
    sums_all[me] = jnp.zeros(sums_all.shape[1:], f32)
    sums_all[me, pl.ds(members, 1), :] = folded(positive, sums_all.shape[2])
    for s in range(1, inner):
        q_moves[s].wait_recv()
        pass_on(s)
    for copy in forwards:
        copy.wait_recv()
    q_group = q_all[...].reshape(members * rows, width)

    summed = None
    for n, s in enumerate([0] + arrivals):
        if s:
            v_moves[s].wait_recv()
        slot = source(along, s, outer) if s else along
        v_block = v_all[slot]
        scores = lax.dot_general(
            v_block, q_group, (((1,), (1,)), ((), ())), preferred_element_type=f32
        )
        raised = jnp.exp2(scores * exponent_scale)
        weights[slot] = raised
        below = jnp.sum(raised, axis=0, keepdims=True)
        summed = below if summed is None else summed + below
        if n == outer - 1:
            for b in range(members):
                sums_all[me, pl.ds(b, 1), :] = summed[:, b * rows : (b + 1) * rows]
            sum_moves = {}
            for step in plane_steps:
                key = plane_key(step)
                sum_moves[step] = send(
                    sums_all.at[me],
                    sums_all.at[me],
                    sum_send.at[key],
                    sum_recv.at[key],
                    plane_peer(step)[1],
                )
        share = lax.dot_general(
            raised.astype(bf16), v_block, (((0,), (0,)), ((), ())), preferred_element_type=f32
        ).reshape(members, rows, width)
        if n == 0:
            q_sum[...] = share
        elif n < outer - 1:
            q_sum[...] += share
        else:
            q_sum[...] += share

    q_moves = {}
    for step in plane_steps[::-1]:
        key = plane_key(step)
        there, device = plane_peer(step)
        q_part[key] = q_sum[there].astype(bf16)
        q_moves[step] = send(q_part.at[key], q_in.at[key], qr_send.at[key], qr_recv.at[key], device)

    for step in plane_steps:
        sum_moves[step].wait_recv()
    message = functools.reduce(jnp.add, [sums_all[i] for i in range(members)])
    total = message[:members]
    inverse = 1.0 / total
    totals[...] = inverse
    log_norm = jnp.log(total)
    gathered_loss = (
        jnp.sum(log_norm, axis=0, keepdims=True)
        - message[members : members + 1] / softmax_sharpness
    )
    losses[along] = jnp.broadcast_to(gathered_loss, losses.shape[1:])
    loss_moves = {}
    for s in line_steps:
        loss_moves[s] = send(
            losses.at[along], losses.at[along], loss_send.at[s], loss_recv.at[s], line_peer(s)[1]
        )
    inverse_row = jnp.concatenate([inverse[b : b + 1] for b in range(members)], axis=1)
    v_moves = {}
    for s in line_steps + [0]:
        slot, device = line_peer(s)
        probs = (weights[slot] * inverse_row).astype(bf16)
        share = jnp.dot(probs, q_group, preferred_element_type=f32)
        if s:
            v_part[s] = share.astype(bf16)
            v_moves[s] = send(v_part.at[s], v_in.at[s], vr_send.at[s], vr_recv.at[s], device)
        else:
            v_own = share
    q_own = q_sum[me]
    for step in plane_steps:
        q_moves[step].wait_recv()
        q_own = q_own + q_in[plane_key(step)].astype(f32)
    own_inverse = jnp.transpose(jnp.broadcast_to(totals[pl.ds(me, 1), :], (rows, rows)))[:, :1]
    q_pull = (q_own * own_inverse - v_all[along].astype(f32))
    q_unit, q_len = unit_rows(q_raw[...])
    q_out[...] = direction_slope(q_pull, q_unit, q_len)

    v_unit, v_len = unit_rows(v_raw[...])
    units[...] = v_unit
    shrink[...] = jnp.broadcast_to(1.0 / v_len, shrink.shape)
    v_sum[...] = v_own - q_all[me].astype(f32)
    for s in line_steps:
        loss_moves[s].wait_recv()
    loss_row = functools.reduce(jnp.add, [losses[i] for i in range(outer)])
    loss_ref[0, 0] = jnp.sum(loss_row[:1]) / batch
    for s in arrivals[:-1]:
        v_moves[s].wait_recv()
        v_sum[...] += v_in[s].astype(f32)
    for s in arrivals[-1:]:
        v_moves[s].wait_recv()
    v_pull = v_sum[...] + v_in[arrivals[-1]].astype(f32)
    v_unit = units[...]
    along_unit = jnp.sum(v_unit * v_pull, axis=1, keepdims=True)
    v_out[...] = (v_pull - v_unit * along_unit) * shrink[...]
    for copy in pending:
        copy.wait_send()


def near_square(count):
    return max(d for d in range(1, math.isqrt(count) + 1) if count % d == 0)


def solution(mesh):
    cores, spots = mesh.shape["blk"], mesh.shape["dp"]
    outer = near_square(spots)
    inner = spots // outer
    members = cores * inner

    def per_device(queries, items):
        rows, width = queries.shape
        f32, bf16 = jnp.float32, jnp.bfloat16
        lanes = rows
        note = members + 8
        dma = pltpu.SemaphoreType.DMA
        vmem = pl.BlockSpec(memory_space=pltpu.VMEM)
        anywhere = pl.BlockSpec(memory_space=pl.ANY)
        loss, q_slope, v_slope = pl.pallas_call(
            functools.partial(kernel, inner, outer, cores),
            out_shape=(
                jax.ShapeDtypeStruct((1, 1), f32),
                pltpu.VMEM((rows, width), f32),
                pltpu.VMEM((rows, width), f32),
            ),
            in_specs=[anywhere, anywhere],
            out_specs=(pl.BlockSpec(memory_space=pltpu.SMEM), vmem, vmem),
            scratch_shapes=[
                pltpu.VMEM((rows, width), bf16),
                pltpu.VMEM((rows, width), bf16),
                pltpu.VMEM((members, rows, width), bf16),
                pltpu.VMEM((outer, rows, width), bf16),
                pltpu.VMEM((outer, rows, members * rows), f32),
                pltpu.VMEM((members, rows, width), f32),
                pltpu.VMEM((members, note, lanes), f32),
                pltpu.VMEM((members, lanes), f32),
                pltpu.VMEM((outer, 8, lanes), f32),
                pltpu.VMEM((members, rows, width), bf16),
                pltpu.VMEM((outer, rows, width), bf16),
                pltpu.VMEM((members, rows, width), bf16),
                pltpu.VMEM((outer, rows, width), bf16),
                pltpu.VMEM((rows, width), f32),
                pltpu.VMEM((rows, width), f32),
                pltpu.VMEM((rows, width), f32),
                dma((2,)),
                dma((inner,)),
                dma((inner,)),
                dma((members,)),
                dma((members,)),
                dma((outer,)),
                dma((outer,)),
                dma((members,)),
                dma((members,)),
                dma((outer,)),
                dma((outer,)),
                dma((members,)),
                dma((members,)),
                dma((outer,)),
                dma((outer,)),
            ],
            compiler_params=pltpu.CompilerParams(
                collective_id=0, has_side_effects=True, vmem_limit_bytes=60 * 1024 * 1024
            ),
        )(queries, items)
        return loss.reshape(()), q_slope / softmax_sharpness, v_slope / softmax_sharpness

    placed = (P(("blk", "dp"), None), P(("blk", "dp"), None))
    return jax.shard_map(
        per_device,
        mesh=mesh,
        in_specs=placed,
        out_specs=(P(), P(("blk", "dp"), None), P(("blk", "dp"), None)),
        check_vma=False,
    )
```
